32 devices in a mesh: branch: 2 (over x), batch: 4 (over y, core), rows: 4 (over z).
Axes of the slice: x: 2, y: 2, z: 4, core: 2. Of those that a mesh axis runs over, the one named last changes fastest.
Arguments:
- timestep: int32 [4], P('batch'), parts along dimension 0, may hold values from 0 to 999
- features: bfloat16 [4, 2, 32, 64, 640], P('batch', 'branch', 'rows'), parts along dimension 0, may hold values from -6 to 6
- conv1_weight: bfloat16 [2, 3, 3, 640, 640], P('branch', None, None, None, 'rows'), may hold values from -0.078125 to 0.078125
- conv1_bias: float32 [2, 640], P('branch'), may hold values from -3 to 3
- conv2_weight: bfloat16 [2, 3, 3, 640, 640], P('branch', None, None, None, 'rows'), may hold values from -0.078125 to 0.078125
- conv2_bias: float32 [2, 640], P('branch'), may hold values from -3 to 3
- norm1_gain: float32 [2, 640], P('branch'), may hold values from 0.25 to 1.75
- norm1_shift: float32 [2, 640], P('branch'), may hold values from -3 to 3
- norm2_gain: float32 [2, 640], P('branch'), may hold values from 0.25 to 1.75
- norm2_shift: float32 [2, 640], P('branch'), may hold values from -3 to 3
- time_weight: bfloat16 [2, 320, 1280], P('branch'), may hold values from -0.3125 to 0.3125
- emb_weight: bfloat16 [2, 1280, 640], P('branch'), may hold values from -0.15625 to 0.15625
- zero_weight: bfloat16 [640, 640], replicated, may hold values from -0.25 to 0.25
- zero_bias: float32 [640], replicated, may hold values from -3 to 3
Outputs:
- block_out: bfloat16 [4, 2, 32, 64, 640], P('batch', 'branch', 'rows'), parts along dimension 0
The draws below stay inside these ranges and needn't reach their ends.
There are 4 independent parts, one for each index of `batch`. The reference program is written for one: setup_inputs(seed, part) draws one part's arguments, and reference() takes and returns one part's arrays. A program takes and returns all parts, laid end to end along the dimension named above; an argument that names none is the same for every part. Nothing has to cross between parts.
All inputs are finite; a program needn't handle non-finite values.
Results may differ from the reference program's by a relative error of at most 0.01.
Values may be sent and summed in bfloat16 or wider, within the bound.
A program may use at most 128 MiB of HBM per device.

```python
import math
import jax
import jax.numpy as jnp
from jax import lax

C = 640
GROUPS = 32
TEMB = 1280
TFREQ = 320
WIDTH = 64
HEIGHT = 32


def levels(stream_key, extent, pieces, low, largest):
    factor_of, own = 1.0, jax.random.fold_in(stream_key, 6)
    for dim, parts in pieces:
        heights = jnp.exp(jax.random.uniform(jax.random.fold_in(own, dim), (parts,), jnp.float32, low / len(pieces), largest / len(pieces)))
        factor_of = factor_of * jnp.repeat(heights, extent[dim] // parts).reshape([-1 if axis == dim else 1 for axis in range(len(extent))])
    return factor_of


def scatter_about(key, shape, scale, bound, pieces=(), kind=jnp.bfloat16):
    array = jax.random.normal(key, shape, jnp.float32) * scale
    if len(pieces) > 0:
        array = levels(key, shape, pieces, -0.22, 0.18) * array
    return jnp.clip(array, min=-bound, max=bound).astype(kind)


def setup_inputs(seed: int = 0, part: int = 0) -> dict:
    streams_of = jax.random.split(jax.random.key(seed), 15)
    part_keys = jax.random.split(jax.random.fold_in(streams_of[14], part), 15)
    timestep = jax.random.randint(part_keys[0], (1,), 0, 1000).astype(jnp.int32)
    features = scatter_about(part_keys[1], (1, 2, HEIGHT, WIDTH, C), 1.0, 6.0, ((1, 2), (2, 4)))
    conv1_weight = scatter_about(streams_of[2], (2, 3, 3, C, C), (9 * C) ** -0.5, 0.078125, ((0, 2), (4, 4)))
    conv1_bias = scatter_about(streams_of[3], (2, C), 0.5, 3.0, ((0, 2),), jnp.float32)
    conv2_weight = scatter_about(streams_of[4], (2, 3, 3, C, C), (9 * C) ** -0.5, 0.078125, ((0, 2), (4, 4)))
    conv2_bias = scatter_about(streams_of[5], (2, C), 0.5, 3.0, ((0, 2),), jnp.float32)
    norm1_gain = jnp.clip(1.0 + 0.15 * jax.random.normal(streams_of[6], (2, C), jnp.float32), 0.25, 1.75)
    norm1_shift = scatter_about(streams_of[7], (2, C), 0.5, 3.0, ((0, 2),), jnp.float32)
    norm2_gain = jnp.clip(1.0 + 0.15 * jax.random.normal(streams_of[8], (2, C), jnp.float32), 0.25, 1.75)
    norm2_shift = scatter_about(streams_of[9], (2, C), 0.5, 3.0, ((0, 2),), jnp.float32)
    time_weight = scatter_about(streams_of[10], (2, TFREQ, TEMB), TFREQ ** -0.5, 0.3125, ((0, 2),))
    emb_weight = scatter_about(streams_of[11], (2, TEMB, C), TEMB ** -0.5, 0.15625, ((0, 2),))
    zero_weight = scatter_about(streams_of[12], (C, C), C ** -0.5, 0.25)
    zero_bias = scatter_about(streams_of[13], (C,), 0.5, 3.0, (), jnp.float32)
    return {"timestep": timestep, "features": features, "conv1_weight": conv1_weight, "conv1_bias": conv1_bias, "conv2_weight": conv2_weight, "conv2_bias": conv2_bias, "norm1_gain": norm1_gain, "norm1_shift": norm1_shift, "norm2_gain": norm2_gain, "norm2_shift": norm2_shift, "time_weight": time_weight, "emb_weight": emb_weight, "zero_weight": zero_weight, "zero_bias": zero_bias}


def sinusoid(timestep, count):
    half = count // 2
    freqs = jnp.exp(-math.log(10000.0) * jnp.arange(half, dtype=jnp.float32) / half)
    angles = timestep.astype(jnp.float32)[0] * freqs
    return jnp.concatenate([jnp.cos(angles), jnp.sin(angles)])

def time_shift(timestep, time_weight, emb_weight):
    waves = sinusoid(timestep, time_weight.shape[0])
    inner = jax.nn.silu(jnp.dot(waves, time_weight.astype(jnp.float32), precision=lax.Precision.HIGHEST))
    return jnp.dot(inner, emb_weight.astype(jnp.float32), precision=lax.Precision.HIGHEST)

def group_norm(values, gain, shift):
    rows, cols, chans = values.shape
    grouped = values.reshape(rows, cols, GROUPS, chans // GROUPS)
    mean = lax.optimization_barrier(jnp.mean(grouped, axis=(0, 1, 3)))
    var = lax.optimization_barrier(jnp.mean(grouped * grouped, axis=(0, 1, 3))) - mean * mean
    normed = (grouped - mean[:, None]) * lax.rsqrt(var + 1e-05)[:, None]
    return jax.nn.silu(normed.reshape(values.shape) * gain + shift).astype(jnp.bfloat16)

def convolve(inputs, kernel):
    return lax.conv_general_dilated(inputs[None], kernel, (1, 1), 'SAME', dimension_numbers=('NHWC', 'HWIO', 'NHWC'), preferred_element_type=jnp.float32)[0]

def reference(timestep, features, conv1_weight, conv1_bias, conv2_weight, conv2_bias, norm1_gain, norm1_shift, norm2_gain, norm2_shift, time_weight, emb_weight, zero_weight, zero_bias):
    blocks = []
    for which in range(2):
        inputs = features[0, which]
        extra = time_shift(timestep, time_weight[which], emb_weight[which])
        act = group_norm(inputs.astype(jnp.float32), norm1_gain[which], norm1_shift[which])
        hidden = (convolve(act, conv1_weight[which]) + conv1_bias[which] + extra).astype(jnp.bfloat16)
        act_two = group_norm(hidden.astype(jnp.float32), norm2_gain[which], norm2_shift[which])
        blocks.append(inputs.astype(jnp.float32) + convolve(act_two, conv2_weight[which]) + conv2_bias[which])
    control_out = blocks[0].astype(jnp.bfloat16)
    flat = control_out.reshape(-1, control_out.shape[2])
    control_res = (jnp.dot(flat, zero_weight, preferred_element_type=jnp.float32) + zero_bias).astype(jnp.bfloat16)
    base_out = (blocks[1] + control_res.reshape(control_out.shape).astype(jnp.float32)).astype(jnp.bfloat16)
    return jnp.stack([control_out, base_out])[None]
```

```python
import functools
import math

import jax
import jax.numpy as jnp
from jax import lax
from jax.experimental import pallas as pl
from jax.experimental.pallas import tpu as pltpu
from jax.sharding import PartitionSpec as P

GROUPS = 32
MESH = pl.DeviceIdType.MESH
F32 = jnp.float32
BF16 = jnp.bfloat16


def sinusoid(timestep, count):
    half = count // 2
    freqs = jnp.exp(-math.log(10000.0) * jnp.arange(half, dtype=F32) / half)
    angles = timestep.astype(F32)[0] * freqs
    return jnp.concatenate([jnp.cos(angles), jnp.sin(angles)])


def exact_dot(rows, weight):
    top = rows.astype(BF16)
    rest = rows - top.astype(F32)
    mid = rest.astype(BF16)
    low = (rest - mid.astype(F32)).astype(BF16)
    terms = jnp.concatenate([top.astype(F32), mid.astype(F32), low.astype(F32), jnp.zeros_like(rows)], axis=0)
    out = jnp.dot(terms.astype(BF16), weight, preferred_element_type=F32)
    size = rows.shape[0]
    return out[:size] + out[size : 2 * size] + out[2 * size : 3 * size]


def kernel(
    n,
    nb,
    count,
    feat,
    w1,
    w2,
    vec,
    waves,
    tw,
    ew,
    zw,
    member,
    out,
    wbuf,
    acts,
    halo1,
    hid,
    acc,
    stat1,
    stat2,
    shift,
    ctl,
    own_sem,
    zs,
    zr,
    ys,
    yr,
    ds_,
    dr,
    es,
    er,
    hs,
    hr,
    ss,
    sr,
    cs,
    cr,
):
    me = lax.axis_index("rows")
    bat = lax.axis_index("batch")
    bra = lax.axis_index("branch")
    rows, width, chans = feat.shape
    m = bat % 4
    hi, lo = m // 2, m % 2
    ymate = bat + 2 - 4 * hi
    dmate = bat + 1 - 2 * lo
    rounds = wbuf.shape[0] // 2

    own = [
        pltpu.make_async_copy(w, wbuf.at[pl.ds(9 * i, 9), me], own_sem.at[i])
        for i, w in enumerate((w1, w2))
    ]
    own[0].start()
    own[1].start()

    barrier = pltpu.get_barrier_semaphore()
    peers = [{"rows": (me + k) % n} for k in range(1, n)]
    peers += [{"batch": ymate}, {"batch": dmate}]
    peers += [{"branch": (bra + k) % nb} for k in range(1, nb)]
    for peer in peers:
        pl.semaphore_signal(barrier, inc=1, device_id=peer, device_id_type=MESH)
    pl.semaphore_wait(barrier, len(peers))

    def remote(src, dst, send, recv, to):
        return pltpu.make_async_remote_copy(
            src_ref=src, dst_ref=dst, send_sem=send, recv_sem=recv, device_id=to, device_id_type=MESH
        )

    def slot(r, src, high, low):
        return wbuf.at[2 * r + high, src, low]

    def z_copy(r, src, way):
        ref = slot(r, src, hi, lo)
        return remote(ref, ref, zs.at[way, r, src], zr.at[r, src], {"rows": me + 1 - 2 * way})

    def y_copy(r, src):
        ref = slot(r, src, hi, lo)
        return remote(ref, ref, ys.at[r, src], yr.at[r, src], {"batch": ymate})

    def d_copy(r, src):
        ref = slot(r, src, hi, lo)
        return remote(ref, ref, ds_.at[r, src], dr.at[r, src], {"batch": dmate})

    def e_copy(r, src):
        ref = slot(r, src, 1 - hi, lo)
        return remote(ref, ref, es.at[r, src], er.at[r, src], {"batch": dmate})

    def send_own(r):
        for way in range(2):

            @pl.when(me < n - 1 if way == 0 else me > 0)
            def _():
                z_copy(r, me, way).start()

    def each_source(fn):
        for d in range(1, n):

            @pl.when(me >= d)
            def _():
                fn(me - d, 0)

            @pl.when(me + d < n)
            def _():
                fn(me + d, 1)

    def z_step(r):
        def one(src, way):
            z_copy(r, src, way).wait_recv()

            @pl.when(me < n - 1 if way == 0 else me > 0)
            def _():
                z_copy(r, src, way).start()

            y_copy(r, src).start()
            d_copy(r, src).start()

        each_source(one)

    def y_step(r):
        def one(src, way):
            y_copy(r, src).wait_recv()
            e_copy(r, src).start()

        each_source(one)

    def d_step(r):
        def one(src, way):
            d_copy(r, src).wait_recv()
            e_copy(r, src).wait_recv()

        each_source(one)

    def drain(r):
        def one(src, way):
            @pl.when(me < n - 1 if way == 0 else me > 0)
            def _():
                z_copy(r, src, way).wait_send()

            y_copy(r, src).wait_send()
            d_copy(r, src).wait_send()
            e_copy(r, src).wait_send()

        each_source(one)
        for way in range(2):

            @pl.when(me < n - 1 if way == 0 else me > 0)
            def _():
                z_copy(r, me, way).wait_send()

    def halo(first, last, buf, k):
        up = remote(first, buf.at[rows + 1], hs.at[k, 0], hr.at[k, 0], {"rows": me - 1})
        down = remote(last, buf.at[0], hs.at[k, 1], hr.at[k, 1], {"rows": me + 1})
        return up, down

    def halo_start(pair):
        @pl.when(me > 0)
        def _():
            pair[0].start()

        @pl.when(me < n - 1)
        def _():
            pair[1].start()

    def halo_wait(pair):
        @pl.when(me < n - 1)
        def _():
            pair[0].wait_recv()
            pair[1].wait_send()

        @pl.when(me > 0)
        def _():
            pair[1].wait_recv()
            pair[0].wait_send()

    def stat_copies(buf, k):
        return [
            remote(buf.at[0], buf.at[j], ss.at[k, j], sr.at[k, j], {"rows": (me + j) % n})
            for j in range(1, n)
        ]

    def local_sums(read, buf):
        def step(i, carry):
            v = read(i).astype(F32)
            return carry[0] + jnp.sum(v, axis=0, keepdims=True), carry[1] + jnp.sum(
                v * v, axis=0, keepdims=True
            )

        zero = jnp.zeros((1, chans), F32)
        total, square = lax.fori_loop(0, rows, step, (zero, zero))
        buf[0] = jnp.concatenate([total, square, jnp.zeros((6, chans), F32)], axis=0)

    def activate(buf, stat, gain, offset):
        sums = stat[0]
        for j in range(1, n):
            sums = sums + stat[j]
        grouped = exact_dot(sums, member[...])
        mean = grouped[0:1] / count
        var = grouped[1:2] / count - mean * mean
        scale = lax.rsqrt(var + 1e-05) * gain
        base = offset - mean * scale
        col = lax.broadcasted_iota(jnp.int32, (width, chans), 0)

        def step(i, carry):
            v = buf[i].astype(F32) * scale + base
            v = v / (1.0 + jnp.exp(-v))
            row = me * rows + i
            v = jnp.where((row >= 1) & (row <= n * rows), v, 0.0)
            acts[1, i] = v.astype(BF16)
            acts[0, i] = jnp.where(col == 0, 0.0, pltpu.roll(v, 1, 0)).astype(BF16)
            acts[2, i] = jnp.where(col == width - 1, 0.0, pltpu.roll(v, width - 1, 0)).astype(BF16)
            return carry

        lax.fori_loop(0, rows + 2, step, 0)

    def taps(first, last):
        def step(t, carry):
            k = t % 9
            a = acts[k % 3, pl.ds(k // 3, rows)].reshape(rows * width, chans)
            w = wbuf[t].reshape(chans, chans)
            acc[...] += lax.dot_general(a, w, (((1,), (1,)), ((), ())), preferred_element_type=F32)
            return carry

        lax.fori_loop(first, last, step, 0)

    pair1 = halo(feat.at[0], feat.at[rows - 1], halo1, 0)
    halo_start(pair1)
    local_sums(lambda i: feat[i], stat1)
    stats1 = stat_copies(stat1, 0)
    for copy in stats1:
        copy.start()
    own[0].wait()
    own[1].wait()
    send_own(0)
    send_own(1)

    inner = exact_dot(jnp.broadcast_to(waves[...], (8, waves.shape[1])), tw[...])
    inner = inner / (1.0 + jnp.exp(-inner))
    shift[...] = exact_dot(inner, ew[...])
    acc[...] = jnp.zeros_like(acc)
    for i in range(rows):
        halo1[i + 1] = feat[i]

    def begin():
        halo_wait(pair1)
        for copy in stats1:
            copy.wait()
        activate(halo1, stat1, vec[2:3], vec[3:4])

    pair2 = halo(hid.at[1], hid.at[rows], hid, 1)
    stats2 = stat_copies(stat2, 1)

    def middle():
        bias = vec[0:1] + shift[0:1]

        def step(i, carry):
            at = pl.ds(pl.multiple_of(i * width, width), width)
            hid[i + 1] = (acc[at, :] + bias).astype(BF16)
            acc[at, :] = jnp.zeros((width, chans), F32)
            return carry

        lax.fori_loop(0, rows, step, 0)
        local_sums(lambda i: hid[i + 1], stat2)
        for copy in stats2:
            copy.start()
        halo_start(pair2)

    def second():
        halo_wait(pair2)
        for copy in stats2:
            copy.wait()
        activate(hid, stat2, vec[4:5], vec[5:6])

    for s in range(rounds + 2):
        if s < rounds:
            if 2 <= s + 1 < rounds:
                send_own(s + 1)
            z_step(s)
        if 0 <= s - 1 < rounds:
            y_step(s - 1)
        r = s - 2
        if r == -1:
            begin()
        if r >= 0:
            d_step(r)
            if r < 4:
                taps(2 * r, 2 * r + 2)
            elif r == 4:
                taps(8, 9)
                middle()
            elif r == 5:
                second()
                taps(9, 12)
            else:
                taps(2 * r, 2 * r + 2)

    def ctl_copy(i):
        return remote(out.at[0, 0, pl.ds(2 * i, 2)], ctl.at[pl.ds(2 * i, 2)], cs.at[i], cr.at[i], {"branch": bra + 1})

    @pl.when(bra == 0)
    def _():
        for i in range(rows // 2):
            for k in range(2 * i, 2 * i + 2):
                out[0, 0, k] = (feat[k].astype(F32) + acc[k * width : (k + 1) * width, :] + vec[1:2]).astype(BF16)
            ctl_copy(i).start()
        for i in range(rows // 2):
            ctl_copy(i).wait_send()

    @pl.when(bra == 1)
    def _():
        for i in range(rows // 2):
            ctl_copy(i).wait_recv()
            got = ctl[2 * i : 2 * i + 2].reshape(2 * width, chans)
            res = (jnp.dot(got, zw[...], preferred_element_type=F32) + vec[6:7]).astype(BF16).astype(F32)
            x = feat[2 * i : 2 * i + 2].reshape(2 * width, chans).astype(F32)
            y = x + acc[2 * i * width : (2 * i + 2) * width, :] + vec[1:2] + res
            out[0, 0, pl.ds(2 * i, 2)] = y.astype(BF16).reshape(2, width, chans)

    for r in range(rounds):
        drain(r)


def body(n, nb, *args):
    (timestep, features, w1, b1, w2, b2, g1, s1, g2, s2, tw, ew, zw, zb) = args
    feat = features[0, 0]
    rows, width, chans = feat.shape
    per_group = chans // GROUPS
    count = float(rows * n * width * per_group)
    quarter = w1.shape[4]

    def turned(w):
        return jnp.swapaxes(w[0].reshape(9, chans, quarter), 1, 2).reshape(9, 2, quarter // 2, chans)

    vec = jnp.concatenate([b1, b2, g1, s1, g2, s2, zb[None], jnp.zeros_like(b1)], axis=0)
    waves = sinusoid(timestep, tw.shape[1])[None]
    group = jnp.arange(chans) // per_group
    member = (group[:, None] == group[None, :]).astype(BF16)
    rounds = 9
    dma = pltpu.SemaphoreType.DMA
    vmem = pl.BlockSpec(memory_space=pltpu.VMEM)
    anyspace = pl.BlockSpec(memory_space=pl.ANY)
    return pl.pallas_call(
        functools.partial(kernel, n, nb, count),
        out_shape=jax.ShapeDtypeStruct(features.shape, BF16),
        in_specs=[vmem, anyspace, anyspace] + [vmem] * 6,
        out_specs=vmem,
        scratch_shapes=[
            pltpu.VMEM((18, n, 2, quarter // 2, chans), BF16),
            pltpu.VMEM((3, rows + 2, width, chans), BF16),
            pltpu.VMEM((rows + 2, width, chans), BF16),
            pltpu.VMEM((rows + 2, width, chans), BF16),
            pltpu.VMEM((rows * width, chans), F32),
            pltpu.VMEM((n, 8, chans), F32),
            pltpu.VMEM((n, 8, chans), F32),
            pltpu.VMEM((8, chans), F32),
            pltpu.VMEM((rows, width, chans), BF16),
            dma((2,)),
            dma((2, rounds, n)),
            dma((rounds, n)),
            dma((rounds, n)),
            dma((rounds, n)),
            dma((rounds, n)),
            dma((rounds, n)),
            dma((rounds, n)),
            dma((rounds, n)),
            dma((2, 2)),
            dma((2, 2)),
            dma((2, n)),
            dma((2, n)),
            dma((rows // 2,)),
            dma((rows // 2,)),
        ],
        compiler_params=pltpu.CompilerParams(
            collective_id=0, has_side_effects=True, vmem_limit_bytes=60 * 1024 * 1024
        ),
    )(feat, turned(w1), turned(w2), vec, waves, tw[0], ew[0], zw, member)


def solution(mesh):
    placed = (
        P("batch"),
        P("batch", "branch", "rows", None, None),
        P("branch", None, None, None, "rows"),
        P("branch", None),
        P("branch", None, None, None, "rows"),
        P("branch", None),
        P("branch", None),
        P("branch", None),
        P("branch", None),
        P("branch", None),
        P("branch", None, None),
        P("branch", None, None),
        P(),
        P(),
    )
    return jax.shard_map(
        functools.partial(body, mesh.shape["rows"], mesh.shape["branch"]),
        mesh=mesh,
        in_specs=placed,
        out_specs=P("batch", "branch", "rows", None, None),
        check_vma=False,
    )
```

```python
import functools
import math

import jax
import jax.numpy as jnp
from jax import lax
from jax.experimental import pallas as pl
from jax.experimental.pallas import tpu as pltpu
from jax.sharding import PartitionSpec as P

GROUPS = 32
LEAD = 2
SKEW = 1
MESH = pl.DeviceIdType.MESH
F32 = jnp.float32
BF16 = jnp.bfloat16


def sinusoid(timestep, count):
    half = count // 2
    freqs = jnp.exp(-math.log(10000.0) * jnp.arange(half, dtype=F32) / half)
    angles = timestep.astype(F32)[0] * freqs
    return jnp.concatenate([jnp.cos(angles), jnp.sin(angles)])


def exact_dot(rows, weight):
    top = rows.astype(BF16)
    rest = rows - top.astype(F32)
    mid = rest.astype(BF16)
    low = (rest - mid.astype(F32)).astype(BF16)
    terms = jnp.concatenate([top.astype(F32), mid.astype(F32), low.astype(F32), jnp.zeros_like(rows)], axis=0)
    out = jnp.dot(terms.astype(BF16), weight, preferred_element_type=F32)
    size = rows.shape[0]
    return out[:size] + out[size : 2 * size] + out[2 * size : 3 * size]


def kernel(
    n,
    nb,
    count,
    feat,
    w1,
    w2,
    b1,
    b2,
    g1,
    s1,
    g2,
    s2,
    zb,
    waves,
    tw_hbm,
    ew_hbm,
    zw_hbm,
    out,
    tw,
    ew,
    zw,
    member,
    wbuf,
    acts,
    halo1,
    hid,
    acc,
    stat1,
    stat2,
    shift,
    ctl,
    own_sem,
    zs,
    zr,
    ys,
    yr,
    ds_,
    dr,
    es,
    er,
    hs,
    hr,
    ss,
    sr,
    cs,
    cr,
):
    me = lax.axis_index("rows")
    bat = lax.axis_index("batch")
    bra = lax.axis_index("branch")
    rows, width, chans = feat.shape
    m = bat % 4
    hi, lo = m // 2, m % 2
    ymate = bat + 2 - 4 * hi
    dmate = bat + 1 - 2 * lo
    rounds = wbuf.shape[0] // 2

    own = [
        pltpu.make_async_copy(w, wbuf.at[pl.ds(9 * i, 9), me], own_sem.at[i])
        for i, w in enumerate((w1, w2))
    ]
    own[0].start()
    own[1].start()
    extra = [
        pltpu.make_async_copy(a, b, own_sem.at[2 + i])
        for i, (a, b) in enumerate(((tw_hbm, tw), (ew_hbm, ew), (zw_hbm, zw)))
    ]

    barrier = pltpu.get_barrier_semaphore()
    peers = [{"rows": (me + k) % n} for k in range(1, n)]
    peers += [{"batch": ymate}, {"batch": dmate}]
    peers += [{"branch": (bra + k) % nb} for k in range(1, nb)]
    for peer in peers:
        pl.semaphore_signal(barrier, inc=1, device_id=peer, device_id_type=MESH)
    pl.semaphore_wait(barrier, len(peers))

    def remote(src, dst, send, recv, to):
        return pltpu.make_async_remote_copy(
            src_ref=src, dst_ref=dst, send_sem=send, recv_sem=recv, device_id=to, device_id_type=MESH
        )

    def slot(r, src, high, low):
        return wbuf.at[2 * r + high, src, low]

    def z_copy(r, src, way):
        ref = slot(r, src, hi, lo)
        return remote(ref, ref, zs.at[way, r, src], zr.at[r, src], {"rows": me + 1 - 2 * way})

    def y_copy(r, src):
        ref = slot(r, src, hi, lo)
        return remote(ref, ref, ys.at[r, src], yr.at[r, src], {"batch": ymate})

    def d_copy(r, src):
        ref = slot(r, src, hi, lo)
        return remote(ref, ref, ds_.at[r, src], dr.at[r, src], {"batch": dmate})

    def e_copy(r, src):
        ref = slot(r, src, 1 - hi, lo)
        return remote(ref, ref, es.at[r, src], er.at[r, src], {"batch": dmate})

    def send_own(r):
        for way in range(2):

            @pl.when(me < n - 1 if way == 0 else me > 0)
            def _():
                z_copy(r, me, way).start()

    def at_distance(fn, d):
        @pl.when(me >= d)
        def _():
            fn(me - d, 0)

        @pl.when(me + d < n)
        def _():
            fn(me + d, 1)

    def each_source(fn):
        for d in range(1, n):
            at_distance(fn, d)

    def z_step(r, d):
        def one(src, way):
            z_copy(r, src, way).wait_recv()

            @pl.when(me < n - 1 if way == 0 else me > 0)
            def _():
                z_copy(r, src, way).start()

            y_copy(r, src).start()
            d_copy(r, src).start()

        at_distance(one, d)

    def y_step(r, d):
        def one(src, way):
            y_copy(r, src).wait_recv()
            e_copy(r, src).start()

        at_distance(one, d)

    def d_step(r):
        def one(src, way):
            d_copy(r, src).wait_recv()
            e_copy(r, src).wait_recv()

        each_source(one)

    def drain(r):
        def one(src, way):
            @pl.when(me < n - 1 if way == 0 else me > 0)
            def _():
                z_copy(r, src, way).wait_send()

            y_copy(r, src).wait_send()
            d_copy(r, src).wait_send()
            e_copy(r, src).wait_send()

        each_source(one)
        for way in range(2):

            @pl.when(me < n - 1 if way == 0 else me > 0)
            def _():
                z_copy(r, me, way).wait_send()

    def halo(first, last, buf, k):
        up = remote(first, buf.at[rows + 1], hs.at[k, 0], hr.at[k, 0], {"rows": me - 1})
        down = remote(last, buf.at[0], hs.at[k, 1], hr.at[k, 1], {"rows": me + 1})
        return up, down

    def halo_start(pair):
        @pl.when(me > 0)
        def _():
            pair[0].start()

        @pl.when(me < n - 1)
        def _():
            pair[1].start()

    def halo_wait(pair):
        @pl.when(me < n - 1)
        def _():
            pair[0].wait_recv()
            pair[1].wait_send()

        @pl.when(me > 0)
        def _():
            pair[1].wait_recv()
            pair[0].wait_send()

    def stat_copies(buf, k):
        return [
            remote(buf.at[0], buf.at[j], ss.at[k, j], sr.at[k, j], {"rows": (me + j) % n})
            for j in range(1, n)
        ]

    def local_sums(read, buf):
        def step(i, carry):
            v = read(i).astype(F32)
            return carry[0] + jnp.sum(v, axis=0, keepdims=True), carry[1] + jnp.sum(
                v * v, axis=0, keepdims=True
            )

        zero = jnp.zeros((1, chans), F32)
        total, square = lax.fori_loop(0, rows, step, (zero, zero))
        buf[0] = jnp.concatenate([total, square, jnp.zeros((6, chans), F32)], axis=0)

    def activate(buf, stat, gain, offset):
        sums = stat[0]
        for j in range(1, n):
            sums = sums + stat[j]
        grouped = exact_dot(sums, member[...])
        mean = grouped[0:1] / count
        var = grouped[1:2] / count - mean * mean
        scale = lax.rsqrt(var + 1e-05) * gain
        base = offset - mean * scale
        col = lax.broadcasted_iota(jnp.int32, (width, chans), 0)

        def step(i, carry):
            v = buf[i].astype(F32) * scale + base
            v = v / (1.0 + jnp.exp(-v))
            row = me * rows + i
            v = jnp.where((row >= 1) & (row <= n * rows), v, 0.0)
            acts[1, i] = v.astype(BF16)
            acts[0, i] = jnp.where(col == 0, 0.0, pltpu.roll(v, 1, 0)).astype(BF16)
            acts[2, i] = jnp.where(col == width - 1, 0.0, pltpu.roll(v, width - 1, 0)).astype(BF16)
            return carry

        lax.fori_loop(0, rows + 2, step, 0)

    def taps(first, last):
        def step(t, carry):
            k = t % 9
            a = acts[k % 3, pl.ds(k // 3, rows)].reshape(rows * width, chans)
            w = wbuf[t].reshape(chans, chans)
            acc[...] += lax.dot_general(a, w, (((1,), (1,)), ((), ())), preferred_element_type=F32)
            return carry

        lax.fori_loop(first, last, step, 0)

    pair1 = halo(feat.at[0], feat.at[rows - 1], halo1, 0)
    halo_start(pair1)
    own[0].wait()
    for r in range(LEAD):
        send_own(r)
    for copy in extra:
        copy.start()
    local_sums(lambda i: feat[i], stat1)
    stats1 = stat_copies(stat1, 0)
    for copy in stats1:
        copy.start()
    per_group = chans // GROUPS
    low = lax.broadcasted_iota(jnp.int32, (chans, chans), 0)
    high = lax.broadcasted_iota(jnp.int32, (chans, chans), 1)
    same = jnp.floor((low.astype(F32) + 0.5) / per_group) == jnp.floor((high.astype(F32) + 0.5) / per_group)
    member[...] = jnp.where(same, 1.0, 0.0).astype(BF16)
    acc[...] = jnp.zeros_like(acc)
    for i in range(rows):
        halo1[i + 1] = feat[i]

    def time_shift():
        extra[0].wait()
        extra[1].wait()
        inner = exact_dot(jnp.broadcast_to(waves[...], (8, waves.shape[1])), tw[...])
        inner = inner / (1.0 + jnp.exp(-inner))
        shift[...] = exact_dot(inner, ew[...])

    def begin():
        halo_wait(pair1)
        for copy in stats1:
            copy.wait()
        activate(halo1, stat1, g1[...], s1[...])

    pair2 = halo(hid.at[1], hid.at[rows], hid, 1)
    stats2 = stat_copies(stat2, 1)

    def middle():
        bias = b1[...] + shift[0:1]

        def step(i, carry):
            at = pl.ds(pl.multiple_of(i * width, width), width)
            hid[i + 1] = (acc[at, :] + bias).astype(BF16)
            acc[at, :] = jnp.zeros((width, chans), F32)
            return carry

        lax.fori_loop(0, rows, step, 0)
        local_sums(lambda i: hid[i + 1], stat2)
        for copy in stats2:
            copy.start()
        halo_start(pair2)

    def second():
        halo_wait(pair2)
        for copy in stats2:
            copy.wait()
        activate(hid, stat2, g2[...], s2[...])

    def tap(t):
        return lambda: taps(t, t + 1)

    lag = 2 + SKEW * (n - 2)
    plan = {0: [time_shift], 1: [begin]}
    for r in range(rounds):
        plan[r + lag] = [tap(2 * r), tap(2 * r + 1)]
    plan[4 + lag] = [tap(8), middle]
    plan[5 + lag] = [second, tap(9), tap(10), tap(11)]
    for s in range(rounds + lag):
        nxt = s + LEAD
        if nxt < rounds:
            if nxt == max(LEAD, 4):
                own[1].wait()
            send_own(nxt)
        if s >= lag:
            d_step(s - lag)
        work = list(plan.get(s, []))
        for d in range(1, n):
            r = s - SKEW * (d - 1)
            if 0 <= r < rounds:
                z_step(r, d)
            if 0 <= r - 1 < rounds:
                y_step(r - 1, d)
            if work:
                work.pop(0)()
        for unit in work:
            unit()
    extra[2].wait()

    def ctl_copy(i):
        return remote(out.at[0, 0, pl.ds(2 * i, 2)], ctl.at[pl.ds(2 * i, 2)], cs.at[i], cr.at[i], {"branch": bra + 1})

    @pl.when(bra == 0)
    def _():
        for i in range(rows // 2):
            for k in range(2 * i, 2 * i + 2):
                out[0, 0, k] = (feat[k].astype(F32) + acc[k * width : (k + 1) * width, :] + b2[...]).astype(BF16)
            ctl_copy(i).start()
        for i in range(rows // 2):
            ctl_copy(i).wait_send()

    @pl.when(bra == 1)
    def _():
        for i in range(rows // 2):
            ctl_copy(i).wait_recv()
            got = ctl[2 * i : 2 * i + 2].reshape(2 * width, chans)
            res = (jnp.dot(got, zw[...], preferred_element_type=F32) + zb[...]).astype(BF16).astype(F32)
            x = feat[2 * i : 2 * i + 2].reshape(2 * width, chans).astype(F32)
            y = x + acc[2 * i * width : (2 * i + 2) * width, :] + b2[...] + res
            out[0, 0, pl.ds(2 * i, 2)] = y.astype(BF16).reshape(2, width, chans)

    for r in range(rounds):
        drain(r)


def body(n, nb, *args):
    (timestep, features, w1, b1, w2, b2, g1, s1, g2, s2, tw, ew, zw, zb) = args
    feat = features[0, 0]
    rows, width, chans = feat.shape
    per_group = chans // GROUPS
    count = float(rows * n * width * per_group)
    quarter = w1.shape[4]

    def turned(w):
        return jnp.swapaxes(w[0].reshape(9, chans, quarter), 1, 2).reshape(9, 2, quarter // 2, chans)

    waves = sinusoid(timestep, tw.shape[1])[None]
    rounds = 9
    dma = pltpu.SemaphoreType.DMA
    vmem = pl.BlockSpec(memory_space=pltpu.VMEM)
    anyspace = pl.BlockSpec(memory_space=pl.ANY)
    return pl.pallas_call(
        functools.partial(kernel, n, nb, count),
        out_shape=jax.ShapeDtypeStruct(features.shape, BF16),
        in_specs=[vmem, anyspace, anyspace] + [vmem] * 8 + [anyspace] * 3,
        out_specs=vmem,
        scratch_shapes=[
            pltpu.VMEM(tw.shape[1:], BF16),
            pltpu.VMEM(ew.shape[1:], BF16),
            pltpu.VMEM(zw.shape, BF16),
            pltpu.VMEM((chans, chans), BF16),
            pltpu.VMEM((18, n, 2, quarter // 2, chans), BF16),
            pltpu.VMEM((3, rows + 2, width, chans), BF16),
            pltpu.VMEM((rows + 2, width, chans), BF16),
            pltpu.VMEM((rows + 2, width, chans), BF16),
            pltpu.VMEM((rows * width, chans), F32),
            pltpu.VMEM((n, 8, chans), F32),
            pltpu.VMEM((n, 8, chans), F32),
            pltpu.VMEM((8, chans), F32),
            pltpu.VMEM((rows, width, chans), BF16),
            dma((5,)),
            dma((2, rounds, n)),
            dma((rounds, n)),
            dma((rounds, n)),
            dma((rounds, n)),
            dma((rounds, n)),
            dma((rounds, n)),
            dma((rounds, n)),
            dma((rounds, n)),
            dma((2, 2)),
            dma((2, 2)),
            dma((2, n)),
            dma((2, n)),
            dma((rows // 2,)),
            dma((rows // 2,)),
        ],
        compiler_params=pltpu.CompilerParams(
            collective_id=0, has_side_effects=True, vmem_limit_bytes=60 * 1024 * 1024
        ),
    )(feat, turned(w1), turned(w2), b1, b2, g1, s1, g2, s2, zb[None], waves, tw[0], ew[0], zw)


def solution(mesh):
    placed = (
        P("batch"),
        P("batch", "branch", "rows", None, None),
        P("branch", None, None, None, "rows"),
        P("branch", None),
        P("branch", None, None, None, "rows"),
        P("branch", None),
        P("branch", None),
        P("branch", None),
        P("branch", None),
        P("branch", None),
        P("branch", None, None),
        P("branch", None, None),
        P(),
        P(),
    )
    return jax.shard_map(
        functools.partial(body, mesh.shape["rows"], mesh.shape["branch"]),
        mesh=mesh,
        in_specs=placed,
        out_specs=P("batch", "branch", "rows", None, None),
        check_vma=False,
    )
```
